32 devices in a mesh: grp: 4 (over y, x), tp: 8 (over z, core).
Axes of the slice: x: 2, y: 2, z: 4, core: 2. Of those that a mesh axis runs over, the one named last changes fastest.
Arguments:
- key_cache: bfloat16 [4, 8, 768, 512], P('grp', 'tp'), may hold values from -6 to 6
- value_cache: bfloat16 [4, 8, 768, 512], P('grp', 'tp'), may hold values from -12 to 12
- lengths: int32 [4, 8], P('grp', 'tp'), may hold values from 256 to 768, as said below
- queries: bfloat16 [4, 1, 8, 8192], P('grp', None, 'tp'), may hold values from -12 to 12
- new_keys: bfloat16 [4, 1, 8, 512], P('grp', None, 'tp'), may hold values from -18 to 18
- new_values: bfloat16 [4, 1, 8, 512], P('grp', None, 'tp'), may hold values from -12 to 12
- residual: bfloat16 [4, 1, 8, 8192], P('grp', None, 'tp'), may hold values from -4 to 4
- norm_gain: float32 [8192], replicated, may hold values from 0.25 to 1.75
- gate_weight: bfloat16 [4, 13312, 8192], P('grp', 'tp'), may hold values from -0.0625 to 0.0625
- up_weight: bfloat16 [4, 13312, 8192], P('grp', 'tp'), may hold values from -0.0625 to 0.0625
- down_weight: bfloat16 [4, 13312, 8192], P('grp', 'tp'), may hold values from -0.0390625 to 0.0390625
Outputs:
- mixed: bfloat16 [4, 1, 8, 8192], P('grp', None, 'tp')
The draws below stay inside these ranges and needn't reach their ends.
Inputs may be any that keep to these rules, and one draw needn't show every extreme that they name: `lengths`: some row has exactly 768 valid positions.
All inputs are finite; a program needn't handle non-finite values.
Results may differ from the reference program's by a relative error of at most 0.005.
Values may be sent and summed in bfloat16 or wider, within the bound.
A program may use at most 128 MiB of HBM per device.

```python
import jax
import jax.numpy as jnp
from jax import lax

D = 8192
HEADS = 64
HD = 128
KVH = 4
FF = 26624
CAP = 768
STEPS = 1
AGROUPS = 2
GROUP_ROWS = 8
N_GRP = 4


def draw_key_cache(key, part):
    shape = (N_GRP, GROUP_ROWS, CAP, KVH * HD)
    base = jax.random.truncated_normal(jax.random.fold_in(key, 11), -6.0, 6.0, shape)
    return base.astype(jnp.bfloat16)


def draw_queries(key, part):
    shape = (N_GRP, STEPS, GROUP_ROWS, D)
    base = 2.5 * jax.random.truncated_normal(jax.random.fold_in(key, 12), -4.8, 4.8, shape)
    return base.astype(jnp.bfloat16)


def draw_lengths(key, part):
    reach = CAP // 3
    spread = jax.random.randint(jax.random.fold_in(key, 21), (N_GRP, GROUP_ROWS), 0, CAP - reach + 1)
    group = jnp.arange(N_GRP) % (N_GRP // 2)
    length = reach + spread * (group[:, None] + 1) // (N_GRP // 2)
    peak_row = jax.random.randint(jax.random.fold_in(key, 22), (), 0, GROUP_ROWS)
    mark = (jnp.arange(N_GRP)[:, None] == N_GRP // 2 - 1) & (jnp.arange(GROUP_ROWS)[None, :] == peak_row)
    return jnp.where(mark, CAP, length).astype(jnp.int32)


def draw_residual(key, part):
    shape = (N_GRP, STEPS, GROUP_ROWS, D)
    base = jax.random.truncated_normal(jax.random.fold_in(key, 31), -6.0, 6.0, shape)
    return (0.5 * base).astype(jnp.bfloat16)


def levels(own_key, extent, cuts, low, high):
    factor_of = 1.0
    for dim, shards_of in cuts:
        draws = jax.random.uniform(jax.random.fold_in(jax.random.fold_in(own_key, 6), dim), (shards_of,), jnp.float32, low / len(cuts), high / len(cuts))
        factor_of = factor_of * jnp.repeat(jnp.exp(draws), extent[dim] // shards_of).reshape((-1,) + (1,) * (len(extent) - 1 - dim))
    return factor_of


def scatter_about(key, dims, scale, limit, shards=(), held_as=jnp.bfloat16):
    loudness = levels(key, dims, shards, -0.22, 0.18) if shards else 1.0
    values = jax.random.normal(key, dims, jnp.float32) * scale * loudness
    return jnp.minimum(jnp.maximum(values, -limit), limit).astype(held_as)


def setup_inputs(seed: int = 0) -> dict:
    splits = jax.random.split(jax.random.key(seed), 12)
    return {
        "key_cache": draw_key_cache(jax.random.fold_in(splits[11], 71), 0),
        "value_cache": scatter_about(splits[1], (N_GRP, GROUP_ROWS, CAP, KVH * HD), 2.0, 12.0, ((0, 4), (1, 8))),
        "lengths": draw_lengths(jax.random.fold_in(splits[11], 71), 0),
        "queries": draw_queries(jax.random.fold_in(splits[11], 71), 0),
        "new_keys": scatter_about(splits[4], (N_GRP, STEPS, GROUP_ROWS, KVH * HD), 3.0, 18.0, ((0, 4), (2, 8))),
        "new_values": scatter_about(splits[5], (N_GRP, STEPS, GROUP_ROWS, KVH * HD), 2.0, 12.0, ((0, 4), (2, 8))),
        "residual": draw_residual(jax.random.fold_in(splits[11], 71), 0),
        "norm_gain": jnp.clip(1.0 + 0.15 * jax.random.normal(splits[7], (D,), jnp.float32), 0.25, 1.75),
        "gate_weight": scatter_about(splits[8], (N_GRP, FF // AGROUPS, D), D ** -0.5, 0.0625, ((0, 4), (1, 8))),
        "up_weight": scatter_about(splits[9], (N_GRP, FF // AGROUPS, D), D ** -0.5, 0.0625, ((0, 4), (1, 8))),
        "down_weight": scatter_about(splits[10], (N_GRP, FF // AGROUPS, D), FF ** -0.5, 0.0390625, ((0, 4), (1, 8))),
    }


masked_score = -1e+30

def attend_row(row_inputs):
    cache_keys, cache_values, length, query_rows, fresh_keys, fresh_values = row_inputs
    head_share = HEADS // KVH
    score_scale = HD ** (-0.5)
    query_wide = query_rows.astype(jnp.float32).reshape(STEPS, KVH, head_share, HD)
    keys_wide = cache_keys.astype(jnp.float32).reshape(CAP, KVH, HD)
    values_wide = cache_values.astype(jnp.float32).reshape(CAP, KVH, HD)
    fresh_keys_wide = fresh_keys.astype(jnp.float32).reshape(STEPS, KVH, HD)
    fresh_values_wide = fresh_values.astype(jnp.float32).reshape(STEPS, KVH, HD)
    usable = jnp.arange(CAP) < length
    cache_scores = jnp.einsum('sjgd,pjd->sjgp', query_wide, keys_wide) * score_scale
    cache_scores = jnp.where(usable, cache_scores, masked_score)
    causal = jnp.arange(STEPS)[:, None] >= jnp.arange(STEPS)[None, :]
    causal_mask = causal[:, None, None, :]
    fresh_scores = jnp.einsum('sjgd,tjd->sjgt', query_wide, fresh_keys_wide) * score_scale
    fresh_scores = jnp.where(causal_mask, fresh_scores, masked_score)
    ceiling = jnp.maximum(lax.optimization_barrier(jnp.max(cache_scores, axis=-1)), lax.optimization_barrier(jnp.max(fresh_scores, axis=-1)))
    cache_exp = jnp.where(usable, jnp.exp(cache_scores - ceiling[..., None]), 0.0)
    fresh_exp = jnp.where(causal_mask, jnp.exp(fresh_scores - ceiling[..., None]), 0.0)
    denominator = lax.optimization_barrier(jnp.sum(cache_exp, axis=-1)) + lax.optimization_barrier(jnp.sum(fresh_exp, axis=-1))
    cache_weights = lax.optimization_barrier(cache_exp.astype(jnp.bfloat16)).astype(jnp.float32)
    fresh_weights = lax.optimization_barrier(fresh_exp.astype(jnp.bfloat16)).astype(jnp.float32)
    weighted = jnp.einsum('sjgp,pjd->sjgd', cache_weights, values_wide)
    weighted = weighted + jnp.einsum('sjgt,tjd->sjgd', fresh_weights, fresh_values_wide)
    return (weighted / denominator[..., None]).reshape(STEPS, HEADS * HD)

def reference(key_cache, value_cache, lengths, queries, new_keys, new_values, residual, norm_gain, gate_weight, up_weight, down_weight):
    row_total = AGROUPS * GROUP_ROWS
    cache_keys = key_cache[:AGROUPS].reshape(row_total, CAP, KVH * HD)
    cache_values = value_cache[:AGROUPS].reshape(row_total, CAP, KVH * HD)
    row_lengths = lengths[:AGROUPS].reshape(row_total)
    query_rows = jnp.swapaxes(queries[:AGROUPS], 1, 2).reshape(row_total, STEPS, D)
    fresh_keys = jnp.swapaxes(new_keys[:AGROUPS], 1, 2).reshape(row_total, STEPS, KVH * HD)
    fresh_values = jnp.swapaxes(new_values[:AGROUPS], 1, 2).reshape(row_total, STEPS, KVH * HD)
    attended = lax.map(attend_row, (cache_keys, cache_values, row_lengths, query_rows, fresh_keys, fresh_values))
    attended = jnp.swapaxes(attended.reshape(AGROUPS, GROUP_ROWS, STEPS, D), 1, 2)
    hidden = residual[:AGROUPS].astype(jnp.float32) + attended
    spread_sq = lax.optimization_barrier(jnp.mean(hidden * hidden, axis=-1, keepdims=True))
    normed = (hidden * lax.rsqrt(spread_sq + 1e-05) * norm_gain).astype(jnp.bfloat16)
    flat_rows = normed.reshape(-1, D)
    numbers = (((1,), (1,)), ((), ()))
    gate_part = lax.dot_general(flat_rows, gate_weight[AGROUPS:].reshape(FF, D), numbers, preferred_element_type=jnp.float32)
    up_part = lax.dot_general(flat_rows, up_weight[AGROUPS:].reshape(FF, D), numbers, preferred_element_type=jnp.float32)
    product = (jax.nn.silu(gate_part) * up_part).astype(jnp.bfloat16)
    feed = jnp.dot(product, down_weight[AGROUPS:].reshape(FF, D), preferred_element_type=jnp.float32)
    mixed = (hidden + feed.reshape(hidden.shape)).astype(jnp.bfloat16)
    return jnp.concatenate([mixed, jnp.zeros_like(mixed)], axis=0)
```

```python
import functools

import jax
import jax.numpy as jnp
from jax import lax
from jax.experimental import pallas as pl
from jax.experimental.pallas import tpu as pltpu
from jax.sharding import PartitionSpec as P

HEADS = 64
HD = 128
KVH = 4
SHARE = HEADS // KVH
CORES = 2
STRIDE = HEADS + 8

masked_score = -1e30
MESH_ID = pl.DeviceIdType.MESH
VMEM_BYTES = 67_000_000
NT = (((1,), (1,)), ((), ()))
f32 = jnp.float32
bf16 = jnp.bfloat16


def kernel(
    plan,
    lengths,
    gain_hbm,
    queries_hbm,
    fresh_keys_hbm,
    fresh_values_hbm,
    residual_hbm,
    key_hbm,
    value_hbm,
    gate_hbm,
    up_hbm,
    down_hbm,
    out,
    keys,
    values,
    queries,
    fresh_keys,
    fresh_values,
    residual,
    gain,
    hidden,
    normed,
    box,
    wide,
    rows,
    gate_out,
    up_out,
    act,
    keep,
    cross_out,
    cross_in,
    part,
    back,
    slots,
    down_slots,
    cache_sem,
    small_sem,
    slot_sem,
    down_sem,
    row_send,
    row_recv,
    pass_send,
    cross_send,
    cross_recv,
    back_send,
    back_recv,
):
    (half, members, chunk, chunks, ring, down_cols, down_chunks, down_ring, batch) = plan
    peers = half * members
    pairs = peers // CORES
    per_group = members // CORES
    group = lax.axis_index("grp")
    member = lax.axis_index("tp")
    serving = group < half
    core = lax.rem(member, CORES)
    place = member // CORES
    mine = lax.rem(group, half) * per_group + place
    other = jnp.where(serving, half, 0)
    barrier = pltpu.get_barrier_semaphore()
    batches = HEADS // batch
    per_batch = batch * HD // down_cols

    flip = 1 - 2 * (2 * place // per_group)

    def pair_at(i):
        off = per_group - 1 - i // half
        spot = lax.rem(place + off * flip + per_group, per_group)
        side = lax.rem(lax.rem(group, half) + half - 1 - lax.rem(i, half), half)
        return side * per_group + spot

    def twin_id(pair):
        return {
            "grp": other + pair // per_group,
            "tp": lax.rem(pair, per_group) * CORES + core,
        }

    sibling = {"tp": place * CORES + 1 - core}

    def slot_copies(i, s):
        start = pl.multiple_of(i * chunk, chunk)
        return (
            pltpu.make_async_copy(
                gate_hbm.at[0, pl.ds(start, chunk), :], slots.at[s, 0], slot_sem.at[s]
            ),
            pltpu.make_async_copy(
                up_hbm.at[0, pl.ds(start, chunk), :], slots.at[s, 1], slot_sem.at[s]
            ),
        )

    def down_copy(c, s):
        start = pl.multiple_of(c * down_cols, down_cols)
        return pltpu.make_async_copy(
            down_hbm.at[0, :, pl.ds(start, down_cols)], down_slots.at[s], down_sem.at[s]
        )

    small_copies = (
        pltpu.make_async_copy(queries_hbm, queries, small_sem.at[0]),
        pltpu.make_async_copy(fresh_keys_hbm, fresh_keys, small_sem.at[1]),
        pltpu.make_async_copy(fresh_values_hbm, fresh_values, small_sem.at[2]),
        pltpu.make_async_copy(residual_hbm, residual, small_sem.at[3]),
        pltpu.make_async_copy(gain_hbm, gain, small_sem.at[4]),
    )
    key_copy = pltpu.make_async_copy(key_hbm.at[0, 0], keys, cache_sem.at[0])
    value_copy = pltpu.make_async_copy(value_hbm.at[0, 0], values, cache_sem.at[1])

    @pl.when(serving)
    def _():
        small_copies[0].start()
        key_copy.start()
        for copy in small_copies[1:]:
            copy.start()
        value_copy.start()

    @pl.when(jnp.logical_not(serving))
    def _():
        for i in range(ring):
            for copy in slot_copies(i, i):
                copy.start()
        for c in range(down_ring):
            down_copy(c, c).start()

    @pl.loop(0, pairs)
    def _(i):
        pl.semaphore_signal(barrier, inc=1, device_id=twin_id(i), device_id_type=MESH_ID)

    @pl.when(serving)
    def _():
        slot_count = keys.shape[0]
        scale = HD ** (-0.5)
        usable = lax.broadcasted_iota(jnp.int32, (SHARE, slot_count), 1) < lengths[0, 0]
        for copy in small_copies:
            copy.wait()
        key_copy.wait()
        value_copy.wait()
        query = queries[0, 0].astype(f32).reshape(HEADS, HD)
        stream = residual[0, 0].astype(f32).reshape(HEADS, HD)
        own_key = fresh_keys[0, 0].astype(f32).reshape(KVH, HD)
        own_value = fresh_values[0, 0].astype(f32).reshape(KVH, HD)
        spread = jnp.zeros((1, 1), f32)
        for j in range(KVH):
            head = slice(j * SHARE, (j + 1) * SHARE)
            lanes = slice(j * HD, (j + 1) * HD)
            own = query[head, :]
            scores = (
                lax.dot_general(
                    own.astype(bf16), keys[:, lanes], NT, preferred_element_type=f32
                )
                * scale
            )
            scores = jnp.where(usable, scores, masked_score)
            fresh = jnp.sum(own * own_key[j : j + 1, :], axis=-1, keepdims=True) * scale
            ceiling = jnp.maximum(jnp.max(scores, axis=-1, keepdims=True), fresh)
            expo = jnp.where(usable, jnp.exp(scores - ceiling), 0.0)
            fresh_expo = jnp.exp(fresh - ceiling)
            denominator = jnp.sum(expo, axis=-1, keepdims=True) + fresh_expo
            total = jnp.dot(expo.astype(bf16), values[:, lanes], preferred_element_type=f32)
            total = total + fresh_expo.astype(bf16).astype(f32) * own_value[j : j + 1, :]
            row = stream[head, :] + total / denominator
            hidden[head, :] = row
            squares = jnp.sum(row * row, axis=-1, keepdims=True)
            spread = spread + jnp.sum(squares, axis=0, keepdims=True)
        factor = lax.rsqrt(spread / (HEADS * HD) + 1e-05)
        normed[...] = (hidden[...] * factor * gain[...]).astype(bf16)
        pl.semaphore_wait(barrier, pairs)
        row = core * pairs + mine

        @pl.loop(0, pairs)
        def _(i):
            pltpu.make_async_remote_copy(
                src_ref=normed,
                dst_ref=box.at[row],
                send_sem=row_send,
                recv_sem=row_recv.at[row],
                device_id=twin_id(pair_at(i)),
                device_id_type=MESH_ID,
            ).start()

        sent = box.at[pl.ds(0, pairs)]
        pltpu.make_async_copy(sent, sent, row_send).wait()

        for b in range(batches):
            band = slice(b * batch, (b + 1) * batch)
            got = back.at[:, band, :]
            pltpu.make_async_copy(got, got, back_recv.at[b]).wait()
            total = hidden[band, :]
            total = lax.fori_loop(
                0, pairs, lambda p, so_far: so_far + back[p, band, :].astype(f32), total
            )
            out[0, 0, :, b * batch * HD : (b + 1) * batch * HD] = total.reshape(
                1, batch * HD
            ).astype(bf16)

    @pl.when(jnp.logical_not(serving))
    def _():
        out[...] = jnp.zeros_like(out)
        pl.semaphore_signal(barrier, inc=1, device_id=sibling, device_id_type=MESH_ID)
        pl.semaphore_wait(barrier, pairs + 1)

        def widen(row):
            start = pl.multiple_of(row * STRIDE, 8)
            wide[pl.ds(start, HEADS), :] = box[row].astype(f32)

        def arrived(row):
            here = box.at[row]
            pltpu.make_async_copy(here, here, row_recv.at[row]).wait()

        @pl.loop(0, pairs)
        def _(i):
            row = core * pairs + pair_at(i)
            arrived(row)
            pltpu.make_async_remote_copy(
                src_ref=box.at[row],
                dst_ref=box.at[row],
                send_sem=pass_send,
                recv_sem=row_recv.at[row],
                device_id=sibling,
                device_id_type=MESH_ID,
            ).start()
            widen(row)

        @pl.loop(0, pairs)
        def _(i):
            row = (1 - core) * pairs + pair_at(i)
            arrived(row)
            widen(row)

        for h in range(HEADS):
            rows[:, h * HD : (h + 1) * HD] = wide[pl.ds(h, peers, stride=STRIDE), :].astype(bf16)

        sent = box.at[pl.ds(0, pairs)]
        pltpu.make_async_copy(sent, sent, pass_send).wait()

        def hidden_units(start, count):
            at = [lax.rem(start + k, ring) for k in range(count)]
            for s in at:
                pltpu.make_async_copy(slots.at[s], slots.at[s], slot_sem.at[s]).wait()
            for k, s in enumerate(at):
                spot = pl.ds(pl.multiple_of((start + k) * chunk, chunk), chunk)
                if chunks == 1:
                    spot = slice(None)
                for which, store in enumerate((gate_out, up_out)):
                    store[:, spot] = lax.dot_general(
                        rows[...], slots[s, which], NT, preferred_element_type=f32
                    )
            for k, s in enumerate(at):

                @pl.when(start + k + ring < chunks)
                def _():
                    for copy in slot_copies(start + k + ring, s):
                        copy.start()

        step = 2

        @pl.loop(0, chunks // step)
        def _(i):
            hidden_units(i * step, step)

        if chunks % step:
            hidden_units(chunks - chunks % step, chunks % step)

        gate = gate_out[...]
        act[...] = (gate / (1.0 + jnp.exp(-gate)) * up_out[...]).astype(bf16)

        def send_back(g):
            base = pl.multiple_of(g * batch, batch)
            cols = pl.ds(pl.multiple_of(g * batch * HD, batch * HD), batch * HD)
            got = cross_in.at[:, cols]
            pltpu.make_async_copy(got, got, cross_recv.at[g]).wait()
            total = keep[:, cols] + cross_in[:, cols]
            for h in range(batch):
                wide[pl.ds(h, pairs, stride=STRIDE), :] = total[:, h * HD : (h + 1) * HD]
            for r in range(pairs):
                part[r, pl.ds(base, batch), :] = wide[
                    r * STRIDE : r * STRIDE + batch, :
                ].astype(bf16)

            @pl.loop(0, pairs)
            def _(i):
                to = pair_at(i)
                pltpu.make_async_remote_copy(
                    src_ref=part.at[to, pl.ds(base, batch), :],
                    dst_ref=back.at[mine, pl.ds(base, batch), :],
                    send_sem=back_send,
                    recv_sem=back_recv.at[g],
                    device_id=twin_id(to),
                    device_id_type=MESH_ID,
                ).start()

        @pl.loop(0, batches)
        def _(g):
            for k in range(per_batch):
                c = g * per_batch + k
                s = lax.rem(c, down_ring)
                cols = pl.ds(pl.multiple_of(c * down_cols, down_cols), down_cols)
                pltpu.make_async_copy(down_slots.at[s], down_slots.at[s], down_sem.at[s]).wait()
                feed = jnp.dot(act[...], down_slots[s], preferred_element_type=f32)

                @pl.when(c + down_ring < down_chunks)
                def _():
                    down_copy(c + down_ring, s).start()

                low, high = feed[:pairs, :], feed[pairs:, :]
                keep[:, cols] = jnp.where(core == 0, low, high)
                cross_out[:, cols] = jnp.where(core == 0, high, low)

            cols = pl.ds(pl.multiple_of(g * batch * HD, batch * HD), batch * HD)
            pltpu.make_async_remote_copy(
                src_ref=cross_out.at[:, cols],
                dst_ref=cross_in.at[:, cols],
                send_sem=cross_send,
                recv_sem=cross_recv.at[g],
                device_id=sibling,
                device_id_type=MESH_ID,
            ).start()

            @pl.when(g > 0)
            def _():
                send_back(g - 1)

        send_back(batches - 1)
        pltpu.make_async_copy(cross_out, cross_out, cross_send).wait()
        pltpu.make_async_copy(part, part, back_send).wait()


def local(
    key_cache,
    value_cache,
    lengths,
    queries,
    new_keys,
    new_values,
    residual,
    norm_gain,
    gate_weight,
    up_weight,
    down_weight,
):
    groups = lax.axis_size("grp")
    members = lax.axis_size("tp")
    half = groups // 2
    peers = half * members
    pairs = peers // CORES
    width = queries.shape[3]
    slot_count = key_cache.shape[2]
    units = gate_weight.shape[1]
    chunk = HD if units % HD == 0 else units
    chunks = units // chunk
    slot_bytes = 4 * chunk * width
    ring = max(1, min(chunks, 42_000_000 // slot_bytes))
    down_cols = 512
    down_chunks = width // down_cols
    down_ring = min(down_chunks, max(1, 20_500_000 // (2 * units * down_cols)))
    batch = 16
    batches = HEADS // batch
    plan = (half, members, chunk, chunks, ring, down_cols, down_chunks, down_ring, batch)
    vmem = pl.BlockSpec(memory_space=pltpu.VMEM)
    any_space = pl.BlockSpec(memory_space=pl.ANY)
    dma = pltpu.SemaphoreType.DMA
    return pl.pallas_call(
        functools.partial(kernel, plan),
        out_shape=jax.ShapeDtypeStruct(queries.shape, bf16),
        in_specs=[pl.BlockSpec(memory_space=pltpu.SMEM)] + [any_space] * 10,
        out_specs=vmem,
        scratch_shapes=[
            pltpu.VMEM((slot_count, KVH * HD), bf16),
            pltpu.VMEM((slot_count, KVH * HD), bf16),
            pltpu.VMEM(queries.shape, bf16),
            pltpu.VMEM(new_keys.shape, bf16),
            pltpu.VMEM(new_values.shape, bf16),
            pltpu.VMEM(residual.shape, bf16),
            pltpu.VMEM((HEADS, HD), f32),
            pltpu.VMEM((HEADS, HD), f32),
            pltpu.VMEM((HEADS, HD), bf16),
            pltpu.VMEM((peers, HEADS, HD), bf16),
            pltpu.VMEM((peers * STRIDE, HD), f32),
            pltpu.VMEM((peers, width), bf16),
            pltpu.VMEM((peers, units), f32),
            pltpu.VMEM((peers, units), f32),
            pltpu.VMEM((peers, units), bf16),
            pltpu.VMEM((pairs, width), f32),
            pltpu.VMEM((pairs, width), f32),
            pltpu.VMEM((pairs, width), f32),
            pltpu.VMEM((pairs, HEADS, HD), bf16),
            pltpu.VMEM((pairs, HEADS, HD), bf16),
            pltpu.VMEM((ring, 2, chunk, width), bf16),
            pltpu.VMEM((down_ring, units, down_cols), bf16),
            dma((2,)),
            dma((5,)),
            dma((ring,)),
            dma((down_ring,)),
            dma,
            dma((peers,)),
            dma,
            dma,
            dma((batches,)),
            dma,
            dma((batches,)),
        ],
        compiler_params=pltpu.CompilerParams(
            collective_id=0, has_side_effects=True, vmem_limit_bytes=VMEM_BYTES
        ),
    )(
        lengths,
        norm_gain.reshape(HEADS, HD),
        queries,
        new_keys,
        new_values,
        residual,
        key_cache,
        value_cache,
        gate_weight,
        up_weight,
        down_weight,
    )


def solution(mesh):
    return jax.shard_map(
        local,
        mesh=mesh,
        in_specs=(
            P("grp", "tp", None, None),
            P("grp", "tp", None, None),
            P("grp", "tp"),
            P("grp", None, "tp", None),
            P("grp", None, "tp", None),
            P("grp", None, "tp", None),
            P("grp", None, "tp", None),
            P(),
            P("grp", "tp", None),
            P("grp", "tp", None),
            P("grp", "tp", None),
        ),
        out_specs=P("grp", None, "tp", None),
        check_vma=False,
    )
```
